32 devices in a mesh: expert: 4 (over y, x), shard: 8 (over z, core).
Axes of the slice: x: 2, y: 2, z: 4, core: 2. Of those that a mesh axis runs over, the one named last changes fastest.
Arguments:
- master_gate: float32 [64, 2048, 1408], P('expert', 'shard'), may hold values from -0.1875 to 0.1875
- master_up: float32 [64, 2048, 1408], P('expert', 'shard'), may hold values from -0.1875 to 0.1875
- master_down: float32 [64, 1408, 2048], P('expert', None, 'shard'), may hold values from -0.21875 to 0.21875
- router_weight: float32 [2048, 64], P('shard', 'expert'), may hold values from -0.125 to 0.125
- router_gain: float32 [2048], P('shard'), may hold values from 0.25 to 1.75
Outputs:
- final_gate: bfloat16 [64, 2048, 1408], P('expert', None, 'shard')
- final_up: bfloat16 [64, 2048, 1408], P('expert', None, 'shard')
- final_down: bfloat16 [64, 1408, 2048], P('expert', 'shard')
- scale_gate: float32 [64, 1408], P('expert', 'shard')
- scale_up: float32 [64, 1408], P('expert', 'shard')
- scale_down: float32 [64, 1408], P('expert', 'shard')
- serve_router: bfloat16 [2048, 64], replicated
The draws below stay inside these ranges and needn't reach their ends.
All inputs are finite; a program needn't handle non-finite values. Where the reference program divides by a largest or mean magnitude, that divisor is 1e-20 or more.
Results may differ from the reference program's by a relative error of at most 0.001.
Values may be sent and summed in bfloat16 or wider, within the bound.
A program may use at most 256 MiB of HBM per device.

```python
import jax
import jax.numpy as jnp

EXPERTS = 64
D_MODEL = 2048
D_EXPERT = 1408


def with_spikes(drawn, stream_key, source, target, shards_of, factor):
    owner, partner = [(jnp.arange(drawn.shape[position]) // (drawn.shape[position] // shards_of)).reshape([-1 if axis == position else 1 for axis in range(drawn.ndim)]) for position in (source, target)]
    chosen = jax.random.permutation(stream_key, shards_of)[partner]
    strong = (owner == chosen) | (owner == (partner + shards_of // 2) % shards_of)
    return jnp.where(strong, factor * drawn, drawn)


def shard_levels(rng, dims, cuts, low, largest):
    def one(axis_at, blocks):
        heights = jax.random.uniform(jax.random.fold_in(jax.random.fold_in(rng, 6), axis_at), (blocks,), jnp.float32, low / len(cuts), largest / len(cuts))
        return jnp.repeat(jnp.exp(heights), dims[axis_at] // blocks).reshape((-1,) + (1,) * (len(dims) - axis_at - 1))

    gain = one(*cuts[0])
    for cut in cuts[1:]:
        gain = gain * one(*cut)
    return gain


def bell_draw(key, shape, scale, bound, cuts=(), kind=jnp.bfloat16):
    values = jax.random.normal(key, shape, jnp.float32) * scale
    if len(cuts) > 0:
        values = shard_levels(key, shape, cuts, -0.22, 0.18) * values
    return jnp.clip(values, min=-bound, max=bound).astype(kind)


def bell_draw_with(stream_key, shape, scale, most, split, heavy, held_as=jnp.bfloat16):
    array = scale * jax.random.normal(stream_key, shape, jnp.float32)
    if split:
        array = array * shard_levels(stream_key, shape, split, -0.22, 0.18)
    return jnp.clip(with_spikes(array, jax.random.fold_in(stream_key, 3), *heavy), -most, most).astype(held_as)


def setup_inputs(seed: int = 0) -> dict:
    key_list = jax.random.split(jax.random.key(seed), 6)
    master_gate = bell_draw_with(key_list[0], (EXPERTS, D_MODEL, D_EXPERT), D_MODEL ** -0.5, 0.1875, ((0, 4), (1, 8)), (1, 2, 8, 2.0), jnp.float32)
    master_up = bell_draw_with(key_list[1], (EXPERTS, D_MODEL, D_EXPERT), D_MODEL ** -0.5, 0.1875, ((0, 4), (1, 8)), (1, 2, 8, 2.0), jnp.float32)
    master_down = bell_draw_with(key_list[2], (EXPERTS, D_EXPERT, D_MODEL), D_EXPERT ** -0.5, 0.21875, ((0, 4), (2, 8)), (2, 1, 8, 2.0), jnp.float32)
    router_weight = bell_draw(key_list[3], (D_MODEL, EXPERTS), D_MODEL ** -0.5, 0.125, ((0, 8), (1, 4)), jnp.float32)
    router_gain = jnp.clip(1.0 + 0.15 * jax.random.normal(key_list[4], (D_MODEL,), jnp.float32), 0.25, 1.75)
    return dict(master_gate=master_gate, master_up=master_up, master_down=master_down, router_weight=router_weight, router_gain=router_gain)


def reference(master_gate, master_up, master_down, router_weight, router_gain):
    scale_gate = jnp.max(jnp.abs(master_gate), axis=1)
    final_gate = (master_gate / jnp.expand_dims(scale_gate, 1)).astype(jnp.bfloat16)
    scale_up = jnp.max(jnp.abs(master_up), axis=1)
    final_up = (master_up / jnp.expand_dims(scale_up, 1)).astype(jnp.bfloat16)
    scale_down = jnp.max(jnp.abs(master_down), axis=2)
    final_down = (master_down / jnp.expand_dims(scale_down, 2)).astype(jnp.bfloat16)
    serve_router = (router_weight * router_gain[:, None]).astype(jnp.bfloat16)
    return final_gate, final_up, final_down, scale_gate, scale_up, scale_down, serve_router
```

```python
import functools

import jax
import jax.numpy as jnp
from jax import lax
from jax.experimental import pallas as pl
from jax.experimental.pallas import tpu as pltpu
from jax.sharding import PartitionSpec as P

MESH = pl.DeviceIdType.MESH
LANES = 128
PAIR = 2


def kernel(
    n, groups_of_experts, gate, up, down, weight, gain,
    out_gate, out_up, out_down, scales, router,
    wide_max, tall_max, wide, tall, turned, column, stage, local, got, kept, part, rows,
    load_max, load_bulk, msg_send, msg_recv, bulk_send, bulk_recv, own_sem, router_sem,
):
    me = lax.axis_index("shard")
    team = lax.axis_index("expert")
    experts, depth, inner = gate.shape
    block = inner // n
    per_array = experts // PAIR
    total = 3 * per_array
    wide_groups = 2 * per_array
    bits = n.bit_length() - 1
    steps = bits + 1
    ins, outs = (gate, up, down), (out_gate, out_up, out_down)
    core = lax.rem(me, 2)

    def partner(step):
        size = 1 if step == steps - 1 else 2**step
        return me + (1 - 2 * lax.rem(me // size, 2)) * size

    barrier = pltpu.get_barrier_semaphore()
    for d in range(1, n):
        pl.semaphore_signal(barrier, inc=1, device_id={"shard": lax.rem(me + d, n)}, device_id_type=MESH)
    for d in range(1, groups_of_experts):
        pl.semaphore_signal(
            barrier, inc=1, device_id={"expert": lax.rem(team + d, groups_of_experts)}, device_id_type=MESH
        )

    def load(group, wide_buf, tall_buf, sem, act):
        for m in range(3):

            @pl.when(group // per_array == m)
            def _():
                first = lax.rem(group, per_array) * PAIR
                act(pltpu.make_async_copy(ins[m].at[pl.ds(first, PAIR)], tall_buf if m == 2 else wide_buf, sem))

    load(0, wide_max, tall_max, load_max, lambda c: c.start())
    load(0, wide, tall, load_bulk, lambda c: c.start())
    pl.semaphore_wait(barrier, n + groups_of_experts - 2)

    team_rows = pl.ds(pl.multiple_of(team * part.shape[0], part.shape[0]), part.shape[0])
    my_columns = pl.ds(pl.multiple_of(me * depth, depth), depth)
    product = (weight[...] * gain[...]).astype(jnp.bfloat16)
    part[...] = product
    rows[team_rows, my_columns] = product
    for d in range(1, n):
        pltpu.make_async_remote_copy(
            part, rows.at[team_rows, my_columns], router_sem.at[0], router_sem.at[1],
            device_id={"shard": lax.rem(me + d, n)}, device_id_type=MESH,
        ).start()
    router_bytes = rows.at[pl.ds(0, part.shape[0]), pl.ds(0, (n - 1) * depth)]
    team_bytes = rows.at[pl.ds(0, (groups_of_experts - 1) * part.shape[0])]

    def message(step, group):
        source = local.at[group * PAIR + 1 - core] if step == 0 else kept.at[step, group]
        return pltpu.make_async_remote_copy(
            source, got.at[step, group], msg_send.at[step, group], msg_recv.at[step, group],
            device_id={"shard": partner(step)}, device_id_type=MESH,
        )

    def local_max(group):
        load(group, wide_max, tall_max, load_max, lambda c: c.wait())

        @pl.when(group < wide_groups)
        def _():
            for j in range(PAIR):
                for b in range(inner // LANES):
                    lanes = pl.ds(b * LANES, LANES)
                    local[group * PAIR + j, :, lanes] = jnp.max(jnp.abs(wide_max[j, :, lanes]), axis=0, keepdims=True)

        @pl.when(group >= wide_groups)
        def _():
            for j in range(PAIR):
                for b in range(inner // LANES):
                    lanes = pl.ds(b * LANES, LANES)
                    most = jnp.abs(tall_max[j, lanes, pl.ds(0, LANES)])
                    for h in range(1, depth // LANES):
                        most = jnp.maximum(most, jnp.abs(tall_max[j, lanes, pl.ds(h * LANES, LANES)]))
                    local[group * PAIR + j, :, lanes] = jnp.max(most.T, axis=0, keepdims=True)

        @pl.when(group + 1 < total)
        def _():
            load(group + 1, wide_max, tall_max, load_max, lambda c: c.start())

        message(0, group).start()

    def reduce_step(step, group):
        message(step - 1, group).wait_recv()
        held = local[group * PAIR + core] if step == 1 else kept[step - 1, group]
        most = jnp.maximum(held, got[step - 1, group])
        kept[step, group] = most
        if step == steps - 1:
            scales[group * PAIR + core] = most
        message(step, group).start()

    def normalise(j, source, chunk):
        for p in range(n):
            part_rows = pl.ds(p * block, block)
            for h in range(depth // LANES):
                lanes = pl.ds(h * LANES, LANES)
                x = source[part_rows, lanes] if j is None else source[j, part_rows, lanes]
                stage[chunk, p, :, lanes] = (x / column[part_rows]).astype(jnp.bfloat16)

    def bulk(group):
        message(steps - 1, group).wait_recv()
        scales[group * PAIR + 1 - core] = got[steps - 1, group]
        load(group, wide, tall, load_bulk, lambda c: c.wait())

        @pl.loop(0, PAIR)
        def _(j):
            chunk = group * PAIR + j
            for b in range(inner // LANES):
                lanes = pl.ds(b * LANES, LANES)
                column[lanes] = jnp.broadcast_to(scales[chunk, :, lanes], (LANES, LANES)).T

            @pl.when(group < wide_groups)
            def _():
                for b in range(inner // LANES):
                    lanes = pl.ds(b * LANES, LANES)
                    for h in range(depth // LANES):
                        half = pl.ds(h * LANES, LANES)
                        turned[lanes, half] = wide[j, half, lanes].T
                normalise(None, turned, chunk)

            @pl.when(group >= wide_groups)
            def _():
                normalise(j, tall, chunk)

            for m in range(3):

                @pl.when(group // per_array == m)
                def _():
                    place = outs[m].at[chunk - m * experts, :, my_columns]
                    for d in range(n):
                        p = lax.rem(me + n // 2 + d, n)
                        if d == n // 2:
                            pltpu.make_async_copy(stage.at[chunk, me], place, own_sem.at[m]).start()
                        else:
                            pltpu.make_async_remote_copy(
                                stage.at[chunk, p], place, bulk_send.at[m], bulk_recv.at[m],
                                device_id={"shard": p}, device_id_type=MESH,
                            ).start()

        @pl.when(group + 1 < total)
        def _():
            load(group + 1, wide, tall, load_bulk, lambda c: c.start())

    @pl.loop(0, total + steps)
    def _(t):
        for step in reversed(range(1, steps)):

            @pl.when((t >= step) & (t < total + step))
            def _():
                reduce_step(step, t - step)

        @pl.when(t < total)
        def _():
            local_max(t)

        @pl.when(t == 1)
        def _():
            pltpu.make_async_copy(router_bytes, router_bytes, router_sem.at[1]).wait()
            for d in range(1, groups_of_experts):
                pltpu.make_async_remote_copy(
                    rows.at[team_rows], rows.at[team_rows], router_sem.at[2], router_sem.at[3],
                    device_id={"expert": lax.rem(team + d, groups_of_experts)}, device_id_type=MESH,
                ).start()

        @pl.when(t >= steps)
        def _():
            bulk(t - steps)

    pltpu.make_async_copy(router_bytes, router_bytes, router_sem.at[0]).wait()
    for s in (2, 3):
        pltpu.make_async_copy(team_bytes, team_bytes, router_sem.at[s]).wait()
    router[...] = rows[...]

    @pl.loop(0, total)
    def _(group):
        for step in range(steps):
            message(step, group).wait_send()

    for m in range(3):
        sent = outs[m].at[:, :, pl.ds(0, (n - 1) * depth)]
        own = outs[m].at[:, :, pl.ds(0, depth)]
        pltpu.make_async_copy(own, own, own_sem.at[m]).wait()
        pltpu.make_async_copy(sent, sent, bulk_send.at[m]).wait()
        pltpu.make_async_copy(sent, sent, bulk_recv.at[m]).wait()


def plain(master_gate, master_up, master_down, router_weight, router_gain):
    scale_gate, scale_up, scale_down = lax.pmax(
        (
            jnp.max(jnp.abs(master_gate), axis=1),
            jnp.max(jnp.abs(master_up), axis=1),
            jnp.max(jnp.abs(master_down), axis=2),
        ),
        "shard",
    )
    narrow_gate, narrow_up, narrow_down = (
        (master_gate / jnp.expand_dims(scale_gate, 1)).astype(jnp.bfloat16),
        (master_up / jnp.expand_dims(scale_up, 1)).astype(jnp.bfloat16),
        (master_down / jnp.expand_dims(scale_down, 2)).astype(jnp.bfloat16),
    )
    final_gate, final_up = (
        lax.all_to_all(narrow_gate, "shard", split_axis=2, concat_axis=1, tiled=True),
        lax.all_to_all(narrow_up, "shard", split_axis=2, concat_axis=1, tiled=True),
    )
    final_down = lax.all_to_all(narrow_down, "shard", split_axis=1, concat_axis=2, tiled=True)
    scale_gate = lax.dynamic_slice_in_dim(
        scale_gate, lax.axis_index("shard") * final_gate.shape[2], final_gate.shape[2], axis=1
    )
    scale_up = lax.dynamic_slice_in_dim(
        scale_up, lax.axis_index("shard") * final_up.shape[2], final_up.shape[2], axis=1
    )
    scale_down = lax.dynamic_slice_in_dim(
        scale_down, lax.axis_index("shard") * final_down.shape[1], final_down.shape[1], axis=1
    )
    part_router = (router_weight * router_gain[:, None]).astype(jnp.bfloat16)
    row_router = lax.all_gather(part_router, "shard", axis=0, tiled=True)
    serve_router = lax.all_gather(row_router, "expert", axis=1, tiled=True)
    return (final_gate, final_up, final_down, scale_gate, scale_up, scale_down, serve_router)


def solution(mesh):
    n, teams = mesh.shape["shard"], mesh.shape["expert"]

    def body(master_gate, master_up, master_down, router_weight, router_gain):
        experts, depth, inner = master_gate.shape
        block = inner // n
        chunks = 3 * experts
        groups = chunks // PAIR
        steps = n.bit_length()
        columns = router_weight.shape[1]
        fits = depth % LANES == 0 and inner % LANES == 0 and block % 8 == 0
        if n < 4 or n & (n - 1) or experts % PAIR or not fits:
            return plain(master_gate, master_up, master_down, router_weight, router_gain)
        f32, bf16 = jnp.float32, jnp.bfloat16
        dma = pltpu.SemaphoreType.DMA
        final = jax.ShapeDtypeStruct((experts, block, n * depth), bf16)
        hbm, vmem = pl.BlockSpec(memory_space=pl.ANY), pl.BlockSpec(memory_space=pltpu.VMEM)
        gate, up, down, scales, router = pl.pallas_call(
            functools.partial(kernel, n, teams),
            out_shape=(
                final, final, final,
                jax.ShapeDtypeStruct((chunks, 1, inner), f32),
                jax.ShapeDtypeStruct((teams * columns, n * depth), bf16),
            ),
            in_specs=[hbm, hbm, hbm, vmem, vmem],
            out_specs=(hbm, hbm, hbm, vmem, vmem),
            scratch_shapes=[
                pltpu.VMEM((PAIR, depth, inner), f32),
                pltpu.VMEM((PAIR, inner, depth), f32),
                pltpu.VMEM((PAIR, depth, inner), f32),
                pltpu.VMEM((PAIR, inner, depth), f32),
                pltpu.VMEM((inner, depth), f32),
                pltpu.VMEM((inner, LANES), f32),
                pltpu.VMEM((chunks, n, block, depth), bf16),
                pltpu.VMEM((chunks, 1, inner), f32),
                pltpu.VMEM((steps, groups, 1, inner), f32),
                pltpu.VMEM((steps, groups, 1, inner), f32),
                pltpu.VMEM((columns, depth), bf16),
                pltpu.VMEM((teams * columns, n * depth), bf16),
                dma, dma,
                dma((steps, groups)), dma((steps, groups)),
                dma((3,)), dma((3,)), dma((3,)), dma((4,)),
            ],
            compiler_params=pltpu.CompilerParams(
                collective_id=0, has_side_effects=True, vmem_limit_bytes=62 * 1024 * 1024
            ),
        )(master_gate, master_up, master_down, router_weight.T, router_gain[None, :])
        mine = lax.dynamic_slice_in_dim(
            scales.reshape(3, experts, inner), lax.axis_index("shard") * block, block, axis=2
        )
        return (gate.swapaxes(1, 2), up.swapaxes(1, 2), down, mine[0], mine[1], mine[2], router.T)

    return jax.shard_map(
        body,
        mesh=mesh,
        in_specs=(
            P("expert", "shard", None),
            P("expert", "shard", None),
            P("expert", None, "shard"),
            P("shard", "expert"),
            P("shard"),
        ),
        out_specs=(
            P("expert", None, "shard"),
            P("expert", None, "shard"),
            P("expert", "shard", None),
            P("expert", "shard"),
            P("expert", "shard"),
            P("expert", "shard"),
            P(),
        ),
        check_vma=False,
    )
```
